32 devices in a mesh: gx: 8 (over z, y), gy: 4 (over x, core).
Axes of the slice: x: 2, y: 2, z: 4, core: 2. Of those that a mesh axis runs over, the one named last changes fastest.
Arguments:
- checkpoint: float32 [16, 32, 1024], P(None, 'gy', 'gx'), may hold values from -6 to 6
- trajectory: float32 [16, 32, 1024], P(None, 'gy', 'gx'), may hold values from -6 to 6
- adjoint_forcing: float32 [16, 32, 1024], P(None, 'gy', 'gx'), may hold values from -6 to 6
- east_diffusion: float32 [16, 32, 1024], P(None, 'gy', 'gx'), may hold values from 0.1 to 1
- north_diffusion: float32 [16, 32, 1024], P(None, 'gy', 'gx'), may hold values from 0.3 to 3
- east_wind: float32 [16, 32, 1024], P(None, 'gy', 'gx'), may hold values from -0.6 to 0.6
- north_wind: float32 [16, 32, 1024], P(None, 'gy', 'gx'), may hold values from -6 to 6, as said below
- level_diffusion: float32 [16], replicated, may hold values from 0.1 to 1
- damping: float32 [16], replicated, may hold values from 0.2 to 2
- source: float32 [16, 32, 1024], P(None, 'gy', 'gx'), may hold values from -4 to 5
- observations: float32 [16, 32, 1024], P(None, 'gy', 'gx'), may hold values from -6 to 6
- observation_weight: float32 [16, 32, 1024], P(None, 'gy', 'gx'), may hold values from 0.1 to 1
- step_index: int32 [1], replicated, may hold values from 0 to 95
Outputs:
- forward_state: float32 [16, 32, 1024], P(None, 'gy', 'gx')
- forward_residual: float32 [16, 32, 1024], P(None, 'gy', 'gx')
- adjoint_state: float32 [16, 32, 1024], P(None, 'gy', 'gx')
The draws below stay inside these ranges and needn't reach their ends.
Inputs may be any that keep to these rules, and one draw needn't show every extreme that they name: At every face the magnitude of north_wind is at most twice north_diffusion.
All inputs are finite; a program needn't handle non-finite values.
Results may differ from the reference program's by a relative error of at most 0.000091.
Values sent between devices are 32-bit elements; how exact they have to be, the bound alone decides.
A program may use at most 64 MiB of HBM per device.

```python
import math
import jax
import jax.numpy as jnp

LEVELS = 16
OUTER = 2
INNER = 4
DAY_STEPS = 96
NLAT = 32
NLON = 1024


def draw_source(key, part):
    noise = jnp.clip(jax.random.normal(key, (LEVELS, NLAT, NLON), jnp.float32), -4.0, 4.0)
    return noise


def flow_parts(key):
    diffusion_key = jax.random.fold_in(key, 4101)
    speed_key = jax.random.fold_in(key, 4102)
    shape = (LEVELS, NLAT, NLON)
    low_log = math.log(0.3)
    high_log = math.log(3.0)
    speed_ratio = jax.random.uniform(speed_key, shape, jnp.float32, -2.0, 2.0)
    diffusion = jnp.exp(jax.random.uniform(diffusion_key, shape, jnp.float32, low_log, high_log))
    diffusion = jnp.clip(diffusion, 0.3, 3.0)
    speed_ratio = jnp.clip(speed_ratio, -2.0, 2.0)
    return (diffusion, diffusion * speed_ratio)


def draw_north_diffusion(key, part):
    return flow_parts(key)[0]


def draw_north_wind(key, part):
    return flow_parts(key)[1]


def level_of(own_key, shape, shards, low, top_value):
    loudness, own = 1.0, jax.random.fold_in(own_key, 6)
    for position, shards_of in shards:
        heights = jnp.exp(jax.random.uniform(jax.random.fold_in(own, position), (shards_of,), jnp.float32, low / len(shards), top_value / len(shards)))
        loudness = loudness * jnp.repeat(heights, shape[position] // shards_of).reshape([-1 if axis == position else 1 for axis in range(len(shape))])
    return loudness


def scatter_about(stream_key, extent, spread, most, pieces=(), kind=jnp.bfloat16):
    loudness = level_of(stream_key, extent, pieces, -0.22, 0.18) if pieces else 1.0
    values = jax.random.normal(stream_key, extent, jnp.float32) * spread * loudness
    return jnp.minimum(jnp.maximum(values, -most), most).astype(kind)


def setup_inputs(seed: int = 0) -> dict:
    streams_of = jax.random.split(jax.random.key(seed), 14)
    checkpoint = scatter_about(streams_of[0], (LEVELS, NLAT, NLON), 1.0, 6.0, ((1, 4), (2, 8)), jnp.float32)
    trajectory = scatter_about(streams_of[1], (LEVELS, NLAT, NLON), 1.0, 6.0, ((1, 4), (2, 8)), jnp.float32)
    adjoint_forcing = scatter_about(streams_of[2], (LEVELS, NLAT, NLON), 1.0, 6.0, ((1, 4), (2, 8)), jnp.float32)
    east_diffusion = jnp.clip(jnp.exp(math.log(1.0) - 2.3025851 * jax.random.uniform(streams_of[3], (LEVELS, NLAT, NLON), jnp.float32) ** level_of(streams_of[3], (LEVELS, NLAT, NLON), ((1, 4), (2, 8)), -0.2, 0.2)), 0.1, 1.0)
    north_diffusion = draw_north_diffusion(jax.random.fold_in(streams_of[13], 71), 0)
    east_wind = jnp.clip(jax.random.uniform(streams_of[5], (LEVELS, NLAT, NLON), jnp.float32, -0.6, 0.6) * level_of(streams_of[5], (LEVELS, NLAT, NLON), ((1, 4), (2, 8)), -0.4, 0.0), -0.6, 0.6)
    north_wind = draw_north_wind(jax.random.fold_in(streams_of[13], 71), 0)
    level_diffusion = jnp.clip(jnp.exp(jax.random.uniform(streams_of[7], (LEVELS,), jnp.float32, math.log(0.1), math.log(1.0))), 0.1, 1.0)
    damping = jnp.clip(jnp.exp(jax.random.uniform(streams_of[8], (LEVELS,), jnp.float32, math.log(0.2), math.log(2.0))), 0.2, 2.0)
    source = draw_source(jax.random.fold_in(streams_of[13], 71), 0)
    observations = scatter_about(streams_of[10], (LEVELS, NLAT, NLON), 1.0, 6.0, ((1, 4), (2, 8)), jnp.float32)
    observation_weight = jnp.clip(jnp.exp(math.log(1.0) - 2.3025851 * jax.random.uniform(streams_of[11], (LEVELS, NLAT, NLON), jnp.float32) ** level_of(streams_of[11], (LEVELS, NLAT, NLON), ((1, 4), (2, 8)), -0.2, 0.2)), 0.1, 1.0)
    step_index = jax.random.randint(streams_of[12], (1,), 0, DAY_STEPS).astype(jnp.int32)
    return {"checkpoint": checkpoint, "trajectory": trajectory, "adjoint_forcing": adjoint_forcing, "east_diffusion": east_diffusion, "north_diffusion": north_diffusion, "east_wind": east_wind, "north_wind": north_wind, "level_diffusion": level_diffusion, "damping": damping, "source": source, "observations": observations, "observation_weight": observation_weight, "step_index": step_index}


RELAXATION = 0.7


def vertical_part(field, up_coef):
    zero_level = jnp.zeros_like(field[:1])
    padded = jnp.concatenate([zero_level, field, zero_level], axis=0)
    flux = up_coef[:, None, None] * (padded[1:] - padded[:-1])
    return -(flux[1:] - flux[:-1])


def apply_forward(west_east, south_north, field, faces):
    east_coef, east_flow, north_coef, north_flow, up_coef = faces
    flux_east = east_flow * (west_east[..., 1:] + west_east[..., :-1]) * 0.5 - east_coef * (west_east[..., 1:] - west_east[..., :-1])
    flux_north = north_flow * (south_north[:, 1:] + south_north[:, :-1]) * 0.5 - north_coef * (south_north[:, 1:] - south_north[:, :-1])
    return (flux_east[..., 1:] - flux_east[..., :-1]) + (flux_north[:, 1:] - flux_north[:, :-1]) + vertical_part(field, up_coef)


def apply_transposed(west_east, south_north, field, faces):
    east_coef, east_flow, north_coef, north_flow, up_coef = faces
    jump_east = west_east[..., :-1] - west_east[..., 1:]
    lower_east = east_flow * 0.5 + east_coef
    upper_east = east_flow * 0.5 - east_coef
    part_east = jump_east[..., 1:] * lower_east[..., 1:] + jump_east[..., :-1] * upper_east[..., :-1]
    jump_north = south_north[:, :-1] - south_north[:, 1:]
    lower_north = north_flow * 0.5 + north_coef
    upper_north = north_flow * 0.5 - north_coef
    part_north = jump_north[:, 1:] * lower_north[:, 1:] + jump_north[:, :-1] * upper_north[:, :-1]
    return part_east + part_north + vertical_part(field, up_coef)


def diagonal_of(tangent, faces, damping):
    east_coef, east_flow, north_coef, north_flow, up_coef = faces
    total = 1.0 + east_coef[..., 1:] + east_coef[..., :-1] + north_coef[:, 1:] + north_coef[:, :-1]
    total = total + (up_coef[1:] + up_coef[:-1])[:, None, None]
    return total + damping[:, None, None] * (1.0 - tangent * tangent)


def global_faces(east_diffusion, north_diffusion, east_wind, north_wind, level_diffusion):
    levels, lat_rows, lon_cols = east_diffusion.shape
    row_mask = (jnp.arange(lat_rows) < lat_rows - 1).astype(jnp.float32)[None, :, None]
    level_mask = (jnp.arange(levels) < levels - 1).astype(jnp.float32)
    north_masked = north_diffusion * row_mask
    flow_masked = north_wind * row_mask
    zero_row = jnp.zeros_like(north_masked[:, :1])
    east_coef = jnp.concatenate([east_diffusion[..., -1:], east_diffusion], axis=2)
    east_flow = jnp.concatenate([east_wind[..., -1:], east_wind], axis=2)
    north_coef = jnp.concatenate([zero_row, north_masked], axis=1)
    north_flow = jnp.concatenate([zero_row, flow_masked], axis=1)
    up_coef = jnp.concatenate([jnp.zeros_like(level_diffusion[:1]), level_diffusion * level_mask])
    return east_coef, east_flow, north_coef, north_flow, up_coef


def wrap_east(field):
    return jnp.concatenate([field[..., -1:], field, field[..., :1]], axis=2)


def pad_north(field):
    zero_row = jnp.zeros_like(field[:, :1])
    return jnp.concatenate([zero_row, field, zero_row], axis=1)


def reference(checkpoint, trajectory, adjoint_forcing, east_diffusion, north_diffusion, east_wind, north_wind, level_diffusion, damping, source, observations, observation_weight, step_index):
    faces = global_faces(east_diffusion, north_diffusion, east_wind, north_wind, level_diffusion)
    levels, lat_rows, lon_cols = checkpoint.shape
    column = jnp.arange(lon_cols).astype(jnp.float32)
    phase = 2.0 * math.pi * column / lon_cols - 2.0 * math.pi * step_index[0].astype(jnp.float32) / DAY_STEPS
    forcing = source * jnp.cos(phase)[None, None, :]
    damp = damping[:, None, None]

    def operate(field):
        return apply_forward(wrap_east(field), pad_north(field), field, faces)

    def operate_transposed(field):
        return apply_transposed(wrap_east(field), pad_north(field), field, faces)

    state = checkpoint
    for newton_step in range(OUTER):
        tangent = jnp.tanh(state)
        diagonal = diagonal_of(tangent, faces, damping)
        resid = state - checkpoint + operate(state) + damp * tangent - forcing
        delta = -RELAXATION * resid / diagonal
        for inner_step in range(INNER - 1):
            image = delta + operate(delta) + damp * (1.0 - tangent * tangent) * delta
            delta = delta + RELAXATION * (-resid - image) / diagonal
        state = state + delta
    final = state - checkpoint + operate(state) + damp * jnp.tanh(state) - forcing

    tangent_n = jnp.tanh(trajectory)
    diagonal_n = diagonal_of(tangent_n, faces, damping)
    local_n = damp * (1.0 - tangent_n * tangent_n)
    multiplier = jnp.zeros_like(trajectory)
    for newton_step in range(OUTER):
        if newton_step == 0:
            resid = -adjoint_forcing
        else:
            resid = multiplier + operate_transposed(multiplier) + local_n * multiplier - adjoint_forcing
        delta = -RELAXATION * resid / diagonal_n
        for inner_step in range(INNER - 1):
            image = delta + operate_transposed(delta) + local_n * delta
            delta = delta + RELAXATION * (-resid - image) / diagonal_n
        multiplier = multiplier + delta
    adjoint_state = multiplier + observation_weight * (state - observations)
    return state, final, adjoint_state
```

```python
import functools
import math

import jax
import jax.numpy as jnp
from jax import lax
from jax.experimental import pallas as pl
from jax.experimental.pallas import tpu as pltpu
from jax.sharding import PartitionSpec as P

OUTER = 2
INNER = 4
DAY_STEPS = 96
RELAXATION = 0.7
FIELDS = 8

MESH = pl.DeviceIdType.MESH


def east_of(v, lane, lanes):
    r = pltpu.roll(v, lanes - 1, 2)
    return jnp.where(lane == lanes - 1, jnp.concatenate([r[1:], r[:1]], axis=0), r)


def west_of(v, lane, lanes):
    r = pltpu.roll(v, 1, 2)
    return jnp.where(lane == 0, jnp.concatenate([r[1:], r[:1]], axis=0), r)


def kernel(
    nx,
    ny,
    ckpt_h,
    traj_h,
    adjf_h,
    ed_h,
    nd_h,
    ew_h,
    nw_h,
    level_ref,
    damp_ref,
    source_h,
    obs_ref,
    weight_ref,
    step_ref,
    state_out,
    resid_out,
    adj_out,
    raw,
    pack_e,
    pack_w,
    recv_e,
    recv_w,
    pack1_e,
    pack1_w,
    recv1_e,
    recv1_w,
    pack2_e,
    pack2_w,
    recv2_e,
    recv2_w,
    coef,
    cf,
    x0,
    x1,
    x2,
    mu1,
    fw,
    fg,
    fd,
    fa,
    fb,
    aw,
    ag,
    ad,
    aa,
    ab,
    load_sem,
    send0,
    got0,
    sendl,
    gotl,
    send1,
    got1,
    send2,
    got2,
):
    levels, rows, lanes = state_out.shape
    wide = INNER
    ring = 2 * rows
    gx = lax.axis_index("gx")
    gy = lax.axis_index("gy")
    east = lax.rem(gx + 1, nx)
    west = lax.rem(gx + nx - 1, nx)
    has_n = gy < ny - 1
    has_s = gy > 0
    north = gy + 1
    south = gy - 1

    loads = [
        pltpu.make_async_copy(h, raw.at[f, :, pl.ds(0, rows), :], load_sem.at[f])
        for f, h in enumerate((ckpt_h, traj_h, adjf_h, ed_h, nd_h, ew_h, nw_h, source_h))
    ]
    for copy in loads:
        copy.start()

    barrier = pltpu.get_barrier_semaphore()

    zero_tile = jnp.zeros((rows, lanes), jnp.float32)

    def clear(l, carry):
        for f in range(FIELDS):
            raw[f, l, rows:, :] = zero_tile
        x1[l + 1, 0, rows:, :] = zero_tile
        mu1[l + 1, 0, rows:, :] = zero_tile
        x2[l + 1, 0, rows:, :] = zero_tile
        return carry

    lax.fori_loop(0, levels, clear, 0)
    for f in range(FIELDS):
        recv_e[f, rows:, :] = zero_tile
        recv_w[f, rows:, :] = zero_tile
    for f in range(2):
        recv1_e[f, rows:, :] = zero_tile
        recv1_w[f, rows:, :] = zero_tile
    recv2_e[rows:, :] = zero_tile
    recv2_w[rows:, :] = zero_tile
    zero_level = jnp.zeros((2, ring, lanes), jnp.float32)
    for ref in (x0, x1, x2, mu1, fa, fb, aa, ab):
        ref[0] = zero_level
        ref[levels + 1] = zero_level

    def greet(column, row):
        pl.semaphore_signal(barrier, inc=1, device_id={"gx": column, "gy": row}, device_id_type=MESH)

    greet(east, gy)
    greet(west, gy)

    @pl.when(has_n)
    def _():
        greet(gx, north)
        greet(east, north)
        greet(west, north)

    @pl.when(has_s)
    def _():
        greet(gx, south)
        greet(east, south)
        greet(west, south)

    pl.semaphore_wait(
        barrier, 2 + 3 * has_n.astype(jnp.int32) + 3 * has_s.astype(jnp.int32)
    )

    def remote(src, dst, send, got, column, row):
        return pltpu.make_async_remote_copy(
            src_ref=src,
            dst_ref=dst,
            send_sem=send,
            recv_sem=got,
            device_id={"gx": column, "gy": row},
            device_id_type=MESH,
        )

    low = pl.ds(0, wide)
    high = pl.ds(rows - wide, wide)
    from_n = pl.ds(rows, wide)
    from_s = pl.ds(ring - wide, wide)

    def lon_copies(pe, pw, re, rw, send, got):
        main = pl.ds(0, rows)
        return (
            [
                remote(pe, rw.at[..., main, :], send.at[0], got.at[0], east, gy),
                remote(pw, re.at[..., main, :], send.at[1], got.at[1], west, gy),
            ],
            [
                remote(
                    pe.at[..., high, :], rw.at[..., from_s, :], send.at[2], got.at[2], east, north
                ),
                remote(
                    pw.at[..., high, :], re.at[..., from_s, :], send.at[3], got.at[3], west, north
                ),
            ],
            [
                remote(
                    pe.at[..., low, :], rw.at[..., from_n, :], send.at[4], got.at[4], east, south
                ),
                remote(
                    pw.at[..., low, :], re.at[..., from_n, :], send.at[5], got.at[5], west, south
                ),
            ],
        )

    def lat_copies(refs, send, got):
        up = [
            remote(ref.at[..., high, :], ref.at[..., from_s, :], send.at[2 * k], got.at[2 * k], gx, north)
            for k, ref in enumerate(refs)
        ]
        down = [
            remote(ref.at[..., low, :], ref.at[..., from_n, :], send.at[2 * k + 1], got.at[2 * k + 1], gx, south)
            for k, ref in enumerate(refs)
        ]
        return up, down

    def start(up, down):
        if up:

            @pl.when(has_n)
            def _():
                for copy in up:
                    copy.start()

            @pl.when(has_s)
            def _():
                for copy in down:
                    copy.start()

    def arrive(up, down):
        @pl.when(has_s)
        def _():
            for copy in up:
                copy.wait_recv()

        @pl.when(has_n)
        def _():
            for copy in down:
                copy.wait_recv()

    def flush(up, down):
        @pl.when(has_n)
        def _():
            for copy in up:
                copy.wait_send()

        @pl.when(has_s)
        def _():
            for copy in down:
                copy.wait_send()

    lane2 = lax.broadcasted_iota(jnp.int32, (rows, lanes), 1)
    group = lane2 // wide
    laner = lax.broadcasted_iota(jnp.int32, (ring, lanes), 1)
    lane = lax.broadcasted_iota(jnp.int32, (2, ring, lanes), 2)
    side = lax.broadcasted_iota(jnp.int32, (2, ring, lanes), 0)
    row = lax.broadcasted_iota(jnp.int32, (2, ring, lanes), 1)

    def pack(tile, l, pe, pw):
        pe = jnp.where(group == l, pltpu.roll(tile, wide * l + wide, 1), pe)
        pw = jnp.where(group == l, pltpu.roll(tile, wide * l, 1), pw)
        return pe, pw

    def unpack(re, rw, l):
        e = pltpu.roll(re, lanes - wide * l, 1)
        w = pltpu.roll(rw, lanes - wide * l - wide, 1)
        return jnp.where(laner < wide, e, jnp.where(laner >= lanes - wide, w, 0.0))

    lat0 = [
        lat_copies([raw.at[f]], send0.at[pl.ds(2 * f, 2)], got0.at[pl.ds(2 * f, 2)])
        for f in range(FIELDS)
    ]
    for f in range(FIELDS):
        loads[f].wait()
        start(*lat0[f])

    def pack0(l, carry):
        out = []
        for f in range(FIELDS):
            out.extend(pack(raw[f, l, :rows, :], l, carry[2 * f], carry[2 * f + 1]))
        return tuple(out)

    packed = lax.fori_loop(0, levels, pack0, (zero_tile,) * (2 * FIELDS), unroll=True)
    for f in range(FIELDS):
        pack_e[f] = packed[2 * f]
        pack_w[f] = packed[2 * f + 1]
    lon0 = lon_copies(pack_e, pack_w, recv_e, recv_w, sendl.at[pl.ds(0, 6)], gotl.at[pl.ds(0, 6)])
    for copy in lon0[0]:
        copy.start()
    start(*lon0[1:])

    column = jnp.where(side == 0, lane, jnp.where(lane < lanes // 2, lane + lanes, lane - lanes))
    column = (gx * lanes + column).astype(jnp.float32)[:, :1]
    phase = (
        2.0 * math.pi * column / (lanes * nx)
        - 2.0 * math.pi * step_ref[0].astype(jnp.float32) / DAY_STEPS
    )
    heat = jnp.cos(phase)
    row_global = gy * rows + jnp.where(row < rows + wide, row, row - ring)
    open_face = (row_global >= 0) & (row_global < rows * ny - 1)

    def level_terms(l):
        up = jnp.where(l < levels - 1, level_ref[l], 0.0)
        down = jnp.where(l > 0, level_ref[jnp.maximum(l - 1, 0)], 0.0)
        return up, down, damp_ref[l]

    for up, down in lat0:
        arrive(up, down)
    for copy in lon0[0]:
        copy.wait_recv()
    arrive(*lon0[1:])

    def prepare(l, carry):
        def ext(f):
            halo = unpack(recv_e[f], recv_w[f], l)
            return jnp.stack([raw[f, l], halo])

        up, down, damp = level_terms(l)
        de = ext(3)
        fe = 0.5 * ext(5)
        dn = jnp.where(open_face, ext(4), 0.0)
        fn = jnp.where(open_face, 0.5 * ext(6), 0.0)
        a, b = fe + de, fe - de
        an, bn = fn + dn, fn - dn
        a_w = west_of(a, lane, lanes)
        b_w = west_of(b, lane, lanes)
        an_s = pltpu.roll(an, 1, 1)
        bn_s = pltpu.roll(bn, 1, 1)
        diag = 1.0 + (a - b_w) + (an - bn_s) + (up + down)
        total = 1.0 + de + 0.5 * (a_w - b_w) + dn + 0.5 * (an_s - bn_s) + (up + down)
        for k, value in enumerate((a, b, a_w, b_w, an, bn, an_s, bn_s, diag, total)):
            coef[k, l] = value
        x = ext(0)
        x0[l + 1] = x
        cf[l] = x + ext(7) * heat
        t = jnp.tanh(ext(1))
        local = damp * (1.0 - t * t)
        w = RELAXATION / (total + local)
        start_delta = w * ext(2)
        aw[l] = w
        ag[l] = 1.0 - w * (diag + local)
        ad[l] = start_delta
        aa[l + 1] = start_delta
        return carry

    lax.fori_loop(0, levels, prepare, 0, unroll=2)

    def off_forward(ref, l, up, down):
        v = ref[l + 1]
        off = (
            east_of(v, lane, lanes) * coef[1, l]
            - west_of(v, lane, lanes) * coef[2, l]
            + pltpu.roll(v, ring - 1, 1) * coef[5, l]
            - pltpu.roll(v, 1, 1) * coef[6, l]
            - up * ref[l + 2]
            - down * ref[l]
        )
        return v, off

    def off_adjoint(ref, l, up, down):
        v = ref[l + 1]
        off = (
            west_of(v, lane, lanes) * coef[3, l]
            - east_of(v, lane, lanes) * coef[0, l]
            + pltpu.roll(v, 1, 1) * coef[7, l]
            - pltpu.roll(v, ring - 1, 1) * coef[4, l]
            - up * ref[l + 2]
            - down * ref[l]
        )
        return v, off

    def resid_forward(x_ref, l):
        up, down, damp = level_terms(l)
        x, off = off_forward(x_ref, l, up, down)
        t = jnp.tanh(x)
        local = damp * (1.0 - t * t)
        diag = coef[8, l]
        r = x * diag + off + damp * t - cf[l]
        w = RELAXATION / (coef[9, l] + local)
        fw[l] = w
        fg[l] = 1.0 - w * (diag + local)
        fd[l] = -w * r
        fa[l + 1] = -w * r

    def resid_adjoint(m_ref, l):
        up, down, damp = level_terms(l)
        m, off = off_adjoint(m_ref, l, up, down)
        w = aw[l]
        d = carry_forcing[l] - (1.0 - ag[l]) * m - w * off
        ad2[l] = d
        aa[l + 1] = d

    def lin_forward(src, l):
        up, down, _ = level_terms(l)
        v, off = off_forward(src, l, up, down)
        return fg[l] * v + fd[l] - fw[l] * off

    def lin_adjoint(src, l, base):
        up, down, _ = level_terms(l)
        v, off = off_adjoint(src, l, up, down)
        return ag[l] * v + base[l] - aw[l] * off

    carry_forcing = ad
    ad2 = coef.at[9]

    def newton(x_ref, base):
        def sweep(f_src, f_dst, a_src, a_dst):
            def body(l, carry):
                f_dst[l + 1] = lin_forward(f_src, l)
                a_dst[l + 1] = lin_adjoint(a_src, l, base)
                return carry

            lax.fori_loop(0, levels, body, 0, unroll=2)

        pairs = [(fa, fb, aa, ab), (fb, fa, ab, aa)]
        for k in range(INNER - 2):
            sweep(*pairs[k % 2])
        return pairs[(INNER - 2) % 2]

    def first(l, carry):
        resid_forward(x0, l)
        return carry

    lax.fori_loop(0, levels, first, 0, unroll=2)
    last = newton(x0, ad)

    def close1(l, carry):
        xe, xw, me, mw = carry
        x = x0[l + 1, 0, :rows, :] + lin_forward(last[0], l)[0, :rows, :]
        m = lin_adjoint(last[2], l, ad)[0, :rows, :]
        x1[l + 1, 0, :rows, :] = x
        mu1[l + 1, 0, :rows, :] = m
        return pack(x, l, xe, xw) + pack(m, l, me, mw)

    xe, xw, me, mw = lax.fori_loop(0, levels, close1, (zero_tile,) * 4, unroll=2)
    pack1_e[0] = xe
    pack1_e[1] = me
    pack1_w[0] = xw
    pack1_w[1] = mw
    inside = pl.ds(1, levels)
    lon1 = lon_copies(
        pack1_e, pack1_w, recv1_e, recv1_w, sendl.at[pl.ds(6, 6)], gotl.at[pl.ds(6, 6)]
    )
    for copy in lon1[0]:
        copy.start()
    start(*lon1[1:])
    lat1 = lat_copies([x1.at[inside, 0], mu1.at[inside, 0]], send1, got1)
    start(*lat1)
    for copy in lon1[0]:
        copy.wait_recv()
    arrive(*lon1[1:])
    arrive(*lat1)

    def spread1(l, carry):
        x1[l + 1, 1] = unpack(recv1_e[0], recv1_w[0], l)
        mu1[l + 1, 1] = unpack(recv1_e[1], recv1_w[1], l)
        return carry

    lax.fori_loop(0, levels, spread1, 0, unroll=4)

    def second(l, carry):
        resid_forward(x1, l)
        resid_adjoint(mu1, l)
        return carry

    lax.fori_loop(0, levels, second, 0, unroll=2)
    last = newton(x1, ad2)

    def close2(l, carry):
        xe, xw = carry
        x = x1[l + 1, 0, :rows, :] + lin_forward(last[0], l)[0, :rows, :]
        m = mu1[l + 1, 0, :rows, :] + lin_adjoint(last[2], l, ad2)[0, :rows, :]
        x2[l + 1, 0, :rows, :] = x
        state_out[l] = x
        adj_out[l] = m + weight_ref[l] * (x - obs_ref[l])
        return pack(x, l, xe, xw)

    xe, xw = lax.fori_loop(0, levels, close2, (zero_tile,) * 2, unroll=2)
    pack2_e[...] = xe
    pack2_w[...] = xw
    main = pl.ds(0, rows)
    lon2 = [
        remote(pack2_e, recv2_w.at[main, :], sendl.at[12], gotl.at[12], east, gy),
        remote(pack2_w, recv2_e.at[main, :], sendl.at[13], gotl.at[13], west, gy),
    ]
    for copy in lon2:
        copy.start()
    lat2 = (
        [
            remote(
                x2.at[inside, 0, pl.ds(rows - 1, 1), :],
                x2.at[inside, 0, pl.ds(ring - 1, 1), :],
                send2.at[0], got2.at[0], gx, north,
            )
        ],
        [
            remote(
                x2.at[inside, 0, pl.ds(0, 1), :],
                x2.at[inside, 0, pl.ds(rows, 1), :],
                send2.at[1], got2.at[1], gx, south,
            )
        ],
    )
    start(*lat2)
    for copy in lon2:
        copy.wait_recv()
    arrive(*lat2)

    def finish(l, carry):
        x2[l + 1, 1] = unpack(recv2_e[...], recv2_w[...], l)
        up, down, damp = level_terms(l)
        x, off = off_forward(x2, l, up, down)
        r = x * coef[8, l] + off + damp * jnp.tanh(x) - cf[l]
        resid_out[l] = r[0, :rows, :]
        return carry

    lax.fori_loop(0, levels, finish, 0, unroll=2)

    for up, down in lat0:
        flush(up, down)
    flush(*lat1)
    flush(*lat2)
    for copy in lon0[0] + lon1[0] + lon2:
        copy.wait_send()
    flush(*lon0[1:])
    flush(*lon1[1:])


def solution(mesh):
    nx, ny = mesh.shape["gx"], mesh.shape["gy"]

    def per_device(*arrays):
        levels, rows, lanes = arrays[0].shape
        assert rows >= INNER and levels * INNER <= lanes
        ring = 2 * rows
        out = jax.ShapeDtypeStruct((levels, rows, lanes), jnp.float32)
        vmem = pl.BlockSpec(memory_space=pltpu.VMEM)
        smem = pl.BlockSpec(memory_space=pltpu.SMEM)
        hbm = pl.BlockSpec(memory_space=pl.ANY)
        f32 = jnp.float32

        def buf(*shape):
            return pltpu.VMEM(shape, f32)

        def padded():
            return buf(levels + 2, 2, ring, lanes)

        def full():
            return buf(levels, 2, ring, lanes)

        def dma(n):
            return pltpu.SemaphoreType.DMA((n,))

        return pl.pallas_call(
            functools.partial(kernel, nx, ny),
            name="step_pair",
            out_shape=(out, out, out),
            in_specs=[hbm] * 7 + [smem, smem, hbm, vmem, vmem, smem],
            out_specs=(vmem, vmem, vmem),
            scratch_shapes=[
                buf(FIELDS, levels, ring, lanes),
                buf(FIELDS, rows, lanes),
                buf(FIELDS, rows, lanes),
                buf(FIELDS, ring, lanes),
                buf(FIELDS, ring, lanes),
                buf(2, rows, lanes),
                buf(2, rows, lanes),
                buf(2, ring, lanes),
                buf(2, ring, lanes),
                buf(rows, lanes),
                buf(rows, lanes),
                buf(ring, lanes),
                buf(ring, lanes),
                buf(10, levels, 2, ring, lanes),
                full(),
                padded(),
                padded(),
                padded(),
                padded(),
                full(),
                full(),
                full(),
                padded(),
                padded(),
                full(),
                full(),
                full(),
                padded(),
                padded(),
                dma(FIELDS),
                dma(2 * FIELDS),
                dma(2 * FIELDS),
                dma(14),
                dma(14),
                dma(4),
                dma(4),
                dma(2),
                dma(2),
            ],
            compiler_params=pltpu.CompilerParams(
                collective_id=0, has_side_effects=True, vmem_limit_bytes=48 * 1024 * 1024
            ),
        )(*arrays)

    block = P(None, "gy", "gx")
    return jax.shard_map(
        per_device,
        mesh=mesh,
        in_specs=(block,) * 7 + (P(), P(), block, block, block, P()),
        out_specs=(block,) * 3,
        check_vma=False,
    )
```

```python
import functools
import math

import jax
import jax.numpy as jnp
from jax import lax
from jax.experimental import pallas as pl
from jax.experimental.pallas import tpu as pltpu
from jax.sharding import PartitionSpec as P

OUTER = 2
INNER = 4
DAY_STEPS = 96
RELAXATION = 0.7
FIELDS = 8

MESH = pl.DeviceIdType.MESH


def east_of(v, lane, lanes):
    r = pltpu.roll(v, lanes - 1, 2)
    return jnp.where(lane == lanes - 1, jnp.concatenate([r[1:], r[:1]], axis=0), r)


def west_of(v, lane, lanes):
    r = pltpu.roll(v, 1, 2)
    return jnp.where(lane == 0, jnp.concatenate([r[1:], r[:1]], axis=0), r)


def kernel(
    nx,
    ny,
    ckpt_h,
    traj_h,
    adjf_h,
    ed_h,
    nd_h,
    ew_h,
    nw_h,
    level_h,
    damp_h,
    source_h,
    obs_h,
    weight_h,
    step_h,
    state_h,
    resid_h,
    adj_h,
    state_out,
    resid_out,
    adj_out,
    raw,
    pack_e,
    pack_w,
    recv_e,
    recv_w,
    pack1_e,
    pack1_w,
    recv1_e,
    recv1_w,
    coef,
    cf,
    x0,
    x1,
    x2,
    mu1,
    fw,
    fg,
    fd,
    fa,
    fb,
    aw,
    ag,
    ad,
    aa,
    ab,
    obs_ref,
    weight_ref,
    level_ref,
    damp_ref,
    step_ref,
    load_sem,
    send0,
    got0,
    sendl,
    gotl,
    send1,
    got1,
    send2,
    got2,
):
    levels, rows, lanes = state_out.shape
    wide = INNER
    span = INNER + 1
    ring = 2 * rows
    gx = lax.axis_index("gx")
    gy = lax.axis_index("gy")
    east = lax.rem(gx + 1, nx)
    west = lax.rem(gx + nx - 1, nx)
    has_n = gy < ny - 1
    has_s = gy > 0
    north = gy + 1
    south = gy - 1

    loads = [
        pltpu.make_async_copy(h, raw.at[f, :, pl.ds(0, rows), :], load_sem.at[f])
        for f, h in enumerate((ckpt_h, traj_h, adjf_h, ed_h, nd_h, ew_h, nw_h, source_h))
    ]
    late_loads = [
        pltpu.make_async_copy(obs_h, obs_ref, load_sem.at[FIELDS]),
        pltpu.make_async_copy(weight_h, weight_ref, load_sem.at[FIELDS + 1]),
    ]
    scalar_loads = [
        pltpu.make_async_copy(level_h, level_ref, load_sem.at[FIELDS + 2]),
        pltpu.make_async_copy(damp_h, damp_ref, load_sem.at[FIELDS + 3]),
        pltpu.make_async_copy(step_h, step_ref, load_sem.at[FIELDS + 4]),
    ]
    for copy in loads + scalar_loads + late_loads:
        copy.start()

    barrier = pltpu.get_barrier_semaphore()

    zero_tile = jnp.zeros((rows, lanes), jnp.float32)

    def clear(l, carry):
        for f in range(FIELDS):
            raw[f, l, rows:, :] = zero_tile
        x1[l + 1, 0, rows:, :] = zero_tile
        mu1[l + 1, 0, rows:, :] = zero_tile
        x2[l + 1, :, rows:, :] = jnp.zeros((2, rows, lanes), jnp.float32)
        return carry

    lax.fori_loop(0, levels, clear, 0)
    for f in range(FIELDS):
        recv_e[f, rows:, :] = zero_tile
        recv_w[f, rows:, :] = zero_tile
    for f in range(2):
        recv1_e[f, rows:, :] = zero_tile
        recv1_w[f, rows:, :] = zero_tile
    zero_level = jnp.zeros((2, ring, lanes), jnp.float32)
    for ref in (x0, x1, x2, mu1, fa, fb, aa, ab):
        ref[0] = zero_level
        ref[levels + 1] = zero_level

    def greet(column, row):
        pl.semaphore_signal(barrier, inc=1, device_id={"gx": column, "gy": row}, device_id_type=MESH)

    greet(east, gy)
    greet(west, gy)

    @pl.when(has_n)
    def _():
        greet(gx, north)
        greet(east, north)
        greet(west, north)

    @pl.when(has_s)
    def _():
        greet(gx, south)
        greet(east, south)
        greet(west, south)

    pl.semaphore_wait(
        barrier, 2 + 3 * has_n.astype(jnp.int32) + 3 * has_s.astype(jnp.int32)
    )

    def remote(src, dst, send, got, column, row):
        return pltpu.make_async_remote_copy(
            src_ref=src,
            dst_ref=dst,
            send_sem=send,
            recv_sem=got,
            device_id={"gx": column, "gy": row},
            device_id_type=MESH,
        )

    low = pl.ds(0, wide)
    high = pl.ds(rows - wide, wide)
    from_n = pl.ds(rows, wide)
    from_s = pl.ds(ring - wide, wide)

    def lon_copies(pe, pw, re, rw, send, got):
        main = pl.ds(0, rows)
        return (
            [
                remote(pe, rw.at[..., main, :], send.at[0], got.at[0], east, gy),
                remote(pw, re.at[..., main, :], send.at[1], got.at[1], west, gy),
            ],
            [
                remote(
                    pe.at[..., high, :], rw.at[..., from_s, :], send.at[2], got.at[2], east, north
                ),
                remote(
                    pw.at[..., high, :], re.at[..., from_s, :], send.at[3], got.at[3], west, north
                ),
            ],
            [
                remote(
                    pe.at[..., low, :], rw.at[..., from_n, :], send.at[4], got.at[4], east, south
                ),
                remote(
                    pw.at[..., low, :], re.at[..., from_n, :], send.at[5], got.at[5], west, south
                ),
            ],
        )

    def lat_copies(refs, send, got):
        up = [
            remote(ref.at[..., high, :], ref.at[..., from_s, :], send.at[2 * k], got.at[2 * k], gx, north)
            for k, ref in enumerate(refs)
        ]
        down = [
            remote(ref.at[..., low, :], ref.at[..., from_n, :], send.at[2 * k + 1], got.at[2 * k + 1], gx, south)
            for k, ref in enumerate(refs)
        ]
        return up, down

    def start(up, down):
        if up:

            @pl.when(has_n)
            def _():
                for copy in up:
                    copy.start()

            @pl.when(has_s)
            def _():
                for copy in down:
                    copy.start()

    def arrive(up, down):
        @pl.when(has_s)
        def _():
            for copy in up:
                copy.wait_recv()

        @pl.when(has_n)
        def _():
            for copy in down:
                copy.wait_recv()

    def flush(up, down):
        @pl.when(has_n)
        def _():
            for copy in up:
                copy.wait_send()

        @pl.when(has_s)
        def _():
            for copy in down:
                copy.wait_send()

    lane2 = lax.broadcasted_iota(jnp.int32, (rows, lanes), 1)
    group = lane2 // span
    laner = lax.broadcasted_iota(jnp.int32, (ring, lanes), 1)
    lane = lax.broadcasted_iota(jnp.int32, (2, ring, lanes), 2)
    side = lax.broadcasted_iota(jnp.int32, (2, ring, lanes), 0)
    row = lax.broadcasted_iota(jnp.int32, (2, ring, lanes), 1)

    def pack(tile, l, pe, pw):
        pe = jnp.where(group == l, pltpu.roll(tile, span * l + span, 1), pe)
        pw = jnp.where(group == l, pltpu.roll(tile, span * l, 1), pw)
        return pe, pw

    def unpack(re, rw, l):
        e = pltpu.roll(re, lanes - span * l, 1)
        w = pltpu.roll(rw, lanes - span * l - span, 1)
        return jnp.where(laner < span, e, jnp.where(laner >= lanes - span, w, 0.0))

    lat0 = [
        lat_copies([raw.at[f]], send0.at[pl.ds(2 * f, 2)], got0.at[pl.ds(2 * f, 2)])
        for f in range(FIELDS)
    ]
    for f in range(FIELDS):
        loads[f].wait()
        start(*lat0[f])

    def pack0(l, carry):
        out = []
        for f in range(FIELDS):
            out.extend(pack(raw[f, l, :rows, :], l, carry[2 * f], carry[2 * f + 1]))
        return tuple(out)

    packed = lax.fori_loop(0, levels, pack0, (zero_tile,) * (2 * FIELDS), unroll=True)
    for f in range(FIELDS):
        pack_e[f] = packed[2 * f]
        pack_w[f] = packed[2 * f + 1]
    lon0 = lon_copies(pack_e, pack_w, recv_e, recv_w, sendl.at[pl.ds(0, 6)], gotl.at[pl.ds(0, 6)])
    for copy in lon0[0]:
        copy.start()
    start(*lon0[1:])

    for copy in scalar_loads:
        copy.wait()
    column = jnp.where(side == 0, lane, jnp.where(lane < lanes // 2, lane + lanes, lane - lanes))
    column = (gx * lanes + column).astype(jnp.float32)[:, :1]
    phase = (
        2.0 * math.pi * column / (lanes * nx)
        - 2.0 * math.pi * step_ref[0].astype(jnp.float32) / DAY_STEPS
    )
    heat = jnp.cos(phase)
    row_global = gy * rows + jnp.where(row < rows + wide, row, row - ring)
    open_face = (row_global >= 0) & (row_global < rows * ny - 1)

    def level_terms(l):
        up = jnp.where(l < levels - 1, level_ref[l], 0.0)
        down = jnp.where(l > 0, level_ref[jnp.maximum(l - 1, 0)], 0.0)
        return up, down, damp_ref[l]

    for up, down in lat0:
        arrive(up, down)
    for copy in lon0[0]:
        copy.wait_recv()
    arrive(*lon0[1:])

    def prepare(l, carry):
        def ext(f):
            halo = unpack(recv_e[f], recv_w[f], l)
            return jnp.stack([raw[f, l], halo])

        up, down, damp = level_terms(l)
        de = ext(3)
        fe = 0.5 * ext(5)
        dn = jnp.where(open_face, ext(4), 0.0)
        fn = jnp.where(open_face, 0.5 * ext(6), 0.0)
        a, b = fe + de, fe - de
        an, bn = fn + dn, fn - dn
        a_w = west_of(a, lane, lanes)
        b_w = west_of(b, lane, lanes)
        an_s = pltpu.roll(an, 1, 1)
        bn_s = pltpu.roll(bn, 1, 1)
        diag = 1.0 + (a - b_w) + (an - bn_s) + (up + down)
        total = 1.0 + de + 0.5 * (a_w - b_w) + dn + 0.5 * (an_s - bn_s) + (up + down)
        for k, value in enumerate((a, b, a_w, b_w, an, bn, an_s, bn_s, diag, total)):
            coef[k, l] = value
        x = ext(0)
        x0[l + 1] = x
        cf[l] = x + ext(7) * heat
        t = jnp.tanh(ext(1))
        local = damp * (1.0 - t * t)
        w = RELAXATION / (total + local)
        start_delta = w * ext(2)
        aw[l] = w
        ag[l] = 1.0 - w * (diag + local)
        ad[l] = start_delta
        aa[l + 1] = start_delta
        return carry

    lax.fori_loop(0, levels, prepare, 0, unroll=4)

    def off_forward(ref, l, up, down):
        v = ref[l + 1]
        off = (
            east_of(v, lane, lanes) * coef[1, l]
            - west_of(v, lane, lanes) * coef[2, l]
            + pltpu.roll(v, ring - 1, 1) * coef[5, l]
            - pltpu.roll(v, 1, 1) * coef[6, l]
            - up * ref[l + 2]
            - down * ref[l]
        )
        return v, off

    def off_adjoint(ref, l, up, down):
        v = ref[l + 1]
        off = (
            west_of(v, lane, lanes) * coef[3, l]
            - east_of(v, lane, lanes) * coef[0, l]
            + pltpu.roll(v, 1, 1) * coef[7, l]
            - pltpu.roll(v, ring - 1, 1) * coef[4, l]
            - up * ref[l + 2]
            - down * ref[l]
        )
        return v, off

    def resid_forward(x_ref, l):
        up, down, damp = level_terms(l)
        x, off = off_forward(x_ref, l, up, down)
        t = jnp.tanh(x)
        local = damp * (1.0 - t * t)
        diag = coef[8, l]
        r = x * diag + off + damp * t - cf[l]
        w = RELAXATION / (coef[9, l] + local)
        fw[l] = w
        fg[l] = 1.0 - w * (diag + local)
        fd[l] = -w * r
        fa[l + 1] = -w * r

    def resid_adjoint(m_ref, l):
        up, down, damp = level_terms(l)
        m, off = off_adjoint(m_ref, l, up, down)
        w = aw[l]
        d = carry_forcing[l] - (1.0 - ag[l]) * m - w * off
        ad2[l] = d
        aa[l + 1] = d

    def lin_forward(src, l):
        up, down, _ = level_terms(l)
        v, off = off_forward(src, l, up, down)
        return fg[l] * v + fd[l] - fw[l] * off

    def lin_adjoint(src, l, base):
        up, down, _ = level_terms(l)
        v, off = off_adjoint(src, l, up, down)
        return ag[l] * v + base[l] - aw[l] * off

    carry_forcing = ad
    ad2 = coef.at[9]

    def newton(x_ref, base):
        def sweep(f_src, f_dst, a_src, a_dst):
            def body(l, carry):
                f_dst[l + 1] = lin_forward(f_src, l)
                a_dst[l + 1] = lin_adjoint(a_src, l, base)
                return carry

            lax.fori_loop(0, levels, body, 0, unroll=4)

        pairs = [(fa, fb, aa, ab), (fb, fa, ab, aa)]
        for k in range(INNER - 2):
            sweep(*pairs[k % 2])
        return pairs[(INNER - 2) % 2]

    def first(l, carry):
        resid_forward(x0, l)
        return carry

    lax.fori_loop(0, levels, first, 0, unroll=4)
    last = newton(x0, ad)

    def close1(l, carry):
        xe, xw, me, mw = carry
        x = x0[l + 1, 0, :rows, :] + lin_forward(last[0], l)[0, :rows, :]
        m = lin_adjoint(last[2], l, ad)[0, :rows, :]
        x1[l + 1, 0, :rows, :] = x
        mu1[l + 1, 0, :rows, :] = m
        return pack(x, l, xe, xw) + pack(m, l, me, mw)

    xe, xw, me, mw = lax.fori_loop(0, levels, close1, (zero_tile,) * 4, unroll=4)
    pack1_e[0] = xe
    pack1_e[1] = me
    pack1_w[0] = xw
    pack1_w[1] = mw
    inside = pl.ds(1, levels)
    lon1 = lon_copies(
        pack1_e, pack1_w, recv1_e, recv1_w, sendl.at[pl.ds(6, 6)], gotl.at[pl.ds(6, 6)]
    )
    for copy in lon1[0]:
        copy.start()
    start(*lon1[1:])
    lat1 = lat_copies([x1.at[inside, 0], mu1.at[inside, 0]], send1, got1)
    start(*lat1)
    for copy in lon1[0]:
        copy.wait_recv()
    arrive(*lon1[1:])
    arrive(*lat1)

    def spread1(l, carry):
        x1[l + 1, 1] = unpack(recv1_e[0], recv1_w[0], l)
        mu1[l + 1, 1] = unpack(recv1_e[1], recv1_w[1], l)
        return carry

    lax.fori_loop(0, levels, spread1, 0, unroll=4)

    def second(l, carry):
        resid_forward(x1, l)
        resid_adjoint(mu1, l)
        return carry

    lax.fori_loop(0, levels, second, 0, unroll=4)
    last = newton(x1, ad2)

    for copy in late_loads:
        copy.wait()

    def close2(l, carry):
        xs = x1[l + 1, :, :rows, :] + lin_forward(last[0], l)[:, :rows, :]
        m = mu1[l + 1, 0, :rows, :] + lin_adjoint(last[2], l, ad2)[0, :rows, :]
        x2[l + 1, 0, :rows, :] = xs[0]
        x2[l + 1, 1, :rows, :] = xs[1]
        x = xs[0]
        state_out[l] = x
        adj_out[l] = m + weight_ref[l] * (x - obs_ref[l])
        return carry

    lax.fori_loop(0, levels, close2, 0, unroll=4)
    lat2 = (
        [
            remote(
                x2.at[inside, 0, pl.ds(rows - 1, 1), :],
                x2.at[inside, 0, pl.ds(ring - 1, 1), :],
                send2.at[0], got2.at[0], gx, north,
            )
        ],
        [
            remote(
                x2.at[inside, 0, pl.ds(0, 1), :],
                x2.at[inside, 0, pl.ds(rows, 1), :],
                send2.at[1], got2.at[1], gx, south,
            )
        ],
    )
    start(*lat2)
    stores = [
        pltpu.make_async_copy(state_out, state_h, load_sem.at[0]),
        pltpu.make_async_copy(adj_out, adj_h, load_sem.at[1]),
        pltpu.make_async_copy(resid_out, resid_h, load_sem.at[2]),
    ]
    stores[0].start()
    stores[1].start()
    arrive(*lat2)

    def finish(l, carry):
        up, down, damp = level_terms(l)
        x, off = off_forward(x2, l, up, down)
        r = x * coef[8, l] + off + damp * jnp.tanh(x) - cf[l]
        resid_out[l] = r[0, :rows, :]
        return carry

    lax.fori_loop(0, levels, finish, 0, unroll=4)
    stores[2].start()

    for up, down in lat0:
        flush(up, down)
    flush(*lat1)
    flush(*lat2)
    for copy in lon0[0] + lon1[0]:
        copy.wait_send()
    flush(*lon0[1:])
    flush(*lon1[1:])
    for copy in stores:
        copy.wait()


def hand_over(a, b, c, x, y, z, held, sem):
    takes = [pltpu.make_async_copy(ref, held.at[k], sem.at[k]) for k, ref in enumerate((a, b, c))]
    gives = [
        pltpu.make_async_copy(held.at[k], ref, sem.at[k + 3]) for k, ref in enumerate((x, y, z))
    ]
    for copy in takes:
        copy.start()
    for take, give in zip(takes, gives):
        take.wait()
        give.start()
    for copy in gives:
        copy.wait()


def solution(mesh):
    nx, ny = mesh.shape["gx"], mesh.shape["gy"]

    def per_device(*arrays):
        levels, rows, lanes = arrays[0].shape
        assert rows >= INNER and levels * (INNER + 1) <= lanes
        ring = 2 * rows
        out = jax.ShapeDtypeStruct((levels, rows, lanes), jnp.float32)
        hbm = pl.BlockSpec(memory_space=pltpu.HBM)
        f32 = jnp.float32

        def buf(*shape):
            return pltpu.VMEM(shape, f32)

        def padded():
            return buf(levels + 2, 2, ring, lanes)

        def full():
            return buf(levels, 2, ring, lanes)

        def dma(n):
            return pltpu.SemaphoreType.DMA((n,))

        results = pl.pallas_call(
            functools.partial(kernel, nx, ny),
            name="step_pair",
            out_shape=(out, out, out),
            in_specs=[hbm] * 13,
            out_specs=(hbm, hbm, hbm),
            scratch_shapes=[
                buf(levels, rows, lanes),
                buf(levels, rows, lanes),
                buf(levels, rows, lanes),
                buf(FIELDS, levels, ring, lanes),
                buf(FIELDS, rows, lanes),
                buf(FIELDS, rows, lanes),
                buf(FIELDS, ring, lanes),
                buf(FIELDS, ring, lanes),
                buf(2, rows, lanes),
                buf(2, rows, lanes),
                buf(2, ring, lanes),
                buf(2, ring, lanes),
                buf(10, levels, 2, ring, lanes),
                full(),
                padded(),
                padded(),
                padded(),
                padded(),
                full(),
                full(),
                full(),
                padded(),
                padded(),
                full(),
                full(),
                full(),
                padded(),
                padded(),
                buf(levels, rows, lanes),
                buf(levels, rows, lanes),
                pltpu.SMEM((levels,), f32),
                pltpu.SMEM((levels,), f32),
                pltpu.SMEM((1,), jnp.int32),
                dma(FIELDS + 5),
                dma(2 * FIELDS),
                dma(2 * FIELDS),
                dma(12),
                dma(12),
                dma(4),
                dma(4),
                dma(2),
                dma(2),
            ],
            compiler_params=pltpu.CompilerParams(
                collective_id=0, has_side_effects=True, vmem_limit_bytes=67043328
            ),
        )(*arrays)
        return pl.pallas_call(
            hand_over,
            name="hand_over",
            out_shape=(out, out, out),
            in_specs=[hbm] * 3,
            out_specs=(hbm, hbm, hbm),
            scratch_shapes=[buf(3, levels, rows, lanes), dma(6)],
            compiler_params=pltpu.CompilerParams(vmem_limit_bytes=67043328),
        )(*results)

    block = P(None, "gy", "gx")
    return jax.shard_map(
        per_device,
        mesh=mesh,
        in_specs=(block,) * 7 + (P(), P(), block, block, block, P()),
        out_specs=(block,) * 3,
        check_vma=False,
    )
```

```python
import functools
import math

import jax
import jax.numpy as jnp
from jax import lax
from jax.experimental import pallas as pl
from jax.experimental.pallas import tpu as pltpu
from jax.sharding import PartitionSpec as P

OUTER = 2
INNER = 4
DAY_STEPS = 96
RELAXATION = 0.7
FIELDS = 8

MESH = pl.DeviceIdType.MESH


def east_of(v, lane, lanes):
    r = pltpu.roll(v, lanes - 1, 2)
    return jnp.where(lane == lanes - 1, jnp.concatenate([r[1:], r[:1]], axis=0), r)


def west_of(v, lane, lanes):
    r = pltpu.roll(v, 1, 2)
    return jnp.where(lane == 0, jnp.concatenate([r[1:], r[:1]], axis=0), r)


def kernel(
    nx,
    ny,
    ckpt_h,
    traj_h,
    adjf_h,
    ed_h,
    nd_h,
    ew_h,
    nw_h,
    level_h,
    damp_h,
    source_h,
    obs_h,
    weight_h,
    step_h,
    state_h,
    resid_h,
    adj_h,
    state_out,
    resid_out,
    adj_out,
    raw,
    pack_e,
    pack_w,
    recv_e,
    recv_w,
    pack1_e,
    pack1_w,
    recv1_e,
    recv1_w,
    coef,
    cf,
    x0,
    x1,
    x2,
    mu1,
    fw,
    fg,
    fd,
    fa,
    fb,
    aw,
    ag,
    ad,
    aa,
    ab,
    obs_ref,
    weight_ref,
    level_ref,
    damp_ref,
    step_ref,
    load_sem,
    send0,
    got0,
    sendl,
    gotl,
    send1,
    got1,
    send2,
    got2,
):
    levels, rows, lanes = state_out.shape
    wide = INNER
    span = INNER + 1
    ring = 2 * rows
    gx = lax.axis_index("gx")
    gy = lax.axis_index("gy")
    east = lax.rem(gx + 1, nx)
    west = lax.rem(gx + nx - 1, nx)
    has_n = gy < ny - 1
    has_s = gy > 0
    north = gy + 1
    south = gy - 1

    loads = [
        pltpu.make_async_copy(h, raw.at[f, :, pl.ds(0, rows), :], load_sem.at[f])
        for f, h in enumerate((ckpt_h, traj_h, adjf_h, ed_h, nd_h, ew_h, nw_h, source_h))
    ]
    late_loads = [
        pltpu.make_async_copy(obs_h, obs_ref, load_sem.at[FIELDS]),
        pltpu.make_async_copy(weight_h, weight_ref, load_sem.at[FIELDS + 1]),
    ]
    scalar_loads = [
        pltpu.make_async_copy(level_h, level_ref, load_sem.at[FIELDS + 2]),
        pltpu.make_async_copy(damp_h, damp_ref, load_sem.at[FIELDS + 3]),
        pltpu.make_async_copy(step_h, step_ref, load_sem.at[FIELDS + 4]),
    ]
    for copy in loads + scalar_loads + late_loads:
        copy.start()

    barrier = pltpu.get_barrier_semaphore()

    zero_tile = jnp.zeros((rows, lanes), jnp.float32)

    def clear(l, carry):
        for f in range(FIELDS):
            raw[f, l, rows:, :] = zero_tile
        x1[l + 1, 0, rows:, :] = zero_tile
        mu1[l + 1, 0, rows:, :] = zero_tile
        x2[l + 1, :, rows:, :] = jnp.zeros((2, rows, lanes), jnp.float32)
        return carry

    lax.fori_loop(0, levels, clear, 0)
    for f in range(FIELDS):
        recv_e[f, rows:, :] = zero_tile
        recv_w[f, rows:, :] = zero_tile
    for f in range(2):
        recv1_e[f, rows:, :] = zero_tile
        recv1_w[f, rows:, :] = zero_tile
    zero_level = jnp.zeros((2, ring, lanes), jnp.float32)
    for ref in (x0, x1, x2, mu1, fa, fb, aa, ab):
        ref[0] = zero_level
        ref[levels + 1] = zero_level

    def greet(column, row):
        pl.semaphore_signal(barrier, inc=1, device_id={"gx": column, "gy": row}, device_id_type=MESH)

    greet(east, gy)
    greet(west, gy)

    @pl.when(has_n)
    def _():
        greet(gx, north)
        greet(east, north)
        greet(west, north)

    @pl.when(has_s)
    def _():
        greet(gx, south)
        greet(east, south)
        greet(west, south)

    pl.semaphore_wait(
        barrier, 2 + 3 * has_n.astype(jnp.int32) + 3 * has_s.astype(jnp.int32)
    )

    def remote(src, dst, send, got, column, row):
        return pltpu.make_async_remote_copy(
            src_ref=src,
            dst_ref=dst,
            send_sem=send,
            recv_sem=got,
            device_id={"gx": column, "gy": row},
            device_id_type=MESH,
        )

    low = pl.ds(0, wide)
    high = pl.ds(rows - wide, wide)
    from_n = pl.ds(rows, wide)
    from_s = pl.ds(ring - wide, wide)

    def lon_copies(pe, pw, re, rw, send, got):
        main = pl.ds(0, rows)
        return (
            [
                remote(pe, rw.at[..., main, :], send.at[0], got.at[0], east, gy),
                remote(pw, re.at[..., main, :], send.at[1], got.at[1], west, gy),
            ],
            [
                remote(
                    pe.at[..., high, :], rw.at[..., from_s, :], send.at[2], got.at[2], east, north
                ),
                remote(
                    pw.at[..., high, :], re.at[..., from_s, :], send.at[3], got.at[3], west, north
                ),
            ],
            [
                remote(
                    pe.at[..., low, :], rw.at[..., from_n, :], send.at[4], got.at[4], east, south
                ),
                remote(
                    pw.at[..., low, :], re.at[..., from_n, :], send.at[5], got.at[5], west, south
                ),
            ],
        )

    def lat_copies(refs, send, got):
        up = [
            remote(ref.at[..., high, :], ref.at[..., from_s, :], send.at[2 * k], got.at[2 * k], gx, north)
            for k, ref in enumerate(refs)
        ]
        down = [
            remote(ref.at[..., low, :], ref.at[..., from_n, :], send.at[2 * k + 1], got.at[2 * k + 1], gx, south)
            for k, ref in enumerate(refs)
        ]
        return up, down

    def start(up, down):
        if up:

            @pl.when(has_n)
            def _():
                for copy in up:
                    copy.start()

            @pl.when(has_s)
            def _():
                for copy in down:
                    copy.start()

    def arrive(up, down):
        @pl.when(has_s)
        def _():
            for copy in up:
                copy.wait_recv()

        @pl.when(has_n)
        def _():
            for copy in down:
                copy.wait_recv()

    def flush(up, down):
        @pl.when(has_n)
        def _():
            for copy in up:
                copy.wait_send()

        @pl.when(has_s)
        def _():
            for copy in down:
                copy.wait_send()

    lane2 = lax.broadcasted_iota(jnp.int32, (rows, lanes), 1)
    group = lane2 // span
    laner = lax.broadcasted_iota(jnp.int32, (ring, lanes), 1)
    lane = lax.broadcasted_iota(jnp.int32, (2, ring, lanes), 2)
    side = lax.broadcasted_iota(jnp.int32, (2, ring, lanes), 0)
    row = lax.broadcasted_iota(jnp.int32, (2, ring, lanes), 1)

    def pack(tile, l, pe, pw):
        pe = jnp.where(group == l, pltpu.roll(tile, span * l + span, 1), pe)
        pw = jnp.where(group == l, pltpu.roll(tile, span * l, 1), pw)
        return pe, pw

    def unpack(re, rw, l):
        e = pltpu.roll(re, lanes - span * l, 1)
        w = pltpu.roll(rw, lanes - span * l - span, 1)
        return jnp.where(laner < span, e, jnp.where(laner >= lanes - span, w, 0.0))

    lat0 = [
        lat_copies([raw.at[f]], send0.at[pl.ds(2 * f, 2)], got0.at[pl.ds(2 * f, 2)])
        for f in range(FIELDS)
    ]
    for f in range(FIELDS):
        loads[f].wait()
        start(*lat0[f])

    def pack0(l, carry):
        out = []
        for f in range(FIELDS):
            out.extend(pack(raw[f, l, :rows, :], l, carry[2 * f], carry[2 * f + 1]))
        return tuple(out)

    packed = lax.fori_loop(0, levels, pack0, (zero_tile,) * (2 * FIELDS), unroll=True)
    for f in range(FIELDS):
        pack_e[f] = packed[2 * f]
        pack_w[f] = packed[2 * f + 1]
    lon0 = lon_copies(pack_e, pack_w, recv_e, recv_w, sendl.at[pl.ds(0, 6)], gotl.at[pl.ds(0, 6)])
    for copy in lon0[0]:
        copy.start()
    start(*lon0[1:])

    for copy in scalar_loads:
        copy.wait()
    column = jnp.where(side == 0, lane, jnp.where(lane < lanes // 2, lane + lanes, lane - lanes))
    column = (gx * lanes + column).astype(jnp.float32)[:, :1]
    phase = (
        2.0 * math.pi * column / (lanes * nx)
        - 2.0 * math.pi * step_ref[0].astype(jnp.float32) / DAY_STEPS
    )
    heat = jnp.cos(phase)
    row_global = gy * rows + jnp.where(row < rows + wide, row, row - ring)
    open_face = (row_global >= 0) & (row_global < rows * ny - 1)

    def level_terms(l):
        up = jnp.where(l < levels - 1, level_ref[l], 0.0)
        down = jnp.where(l > 0, level_ref[jnp.maximum(l - 1, 0)], 0.0)
        return up, down, damp_ref[l]

    for up, down in lat0:
        arrive(up, down)
    for copy in lon0[0]:
        copy.wait_recv()
    arrive(*lon0[1:])

    def prepare(l, carry):
        def ext(f):
            halo = unpack(recv_e[f], recv_w[f], l)
            return jnp.stack([raw[f, l], halo])

        up, down, damp = level_terms(l)
        de = ext(3)
        fe = 0.5 * ext(5)
        dn = jnp.where(open_face, ext(4), 0.0)
        fn = jnp.where(open_face, 0.5 * ext(6), 0.0)
        a, b = fe + de, fe - de
        an, bn = fn + dn, fn - dn
        a_w = west_of(a, lane, lanes)
        b_w = west_of(b, lane, lanes)
        an_s = pltpu.roll(an, 1, 1)
        bn_s = pltpu.roll(bn, 1, 1)
        diag = 1.0 + (a - b_w) + (an - bn_s) + (up + down)
        total = 1.0 + de + 0.5 * (a_w - b_w) + dn + 0.5 * (an_s - bn_s) + (up + down)
        for k, value in enumerate((a, b, a_w, b_w, an, bn, an_s, bn_s, diag, total)):
            coef[k, l] = value
        x = ext(0)
        x0[l + 1] = x
        cf[l] = x + ext(7) * heat
        t = jnp.tanh(ext(1))
        local = damp * (1.0 - t * t)
        w = RELAXATION / (total + local)
        start_delta = w * ext(2)
        aw[l] = w
        ag[l] = 1.0 - w * (diag + local)
        ad[l] = start_delta
        aa[l + 1] = start_delta
        return carry

    lax.fori_loop(0, levels, prepare, 0, unroll=8)

    def off_forward(ref, l, up, down):
        v = ref[l + 1]
        off = (
            east_of(v, lane, lanes) * coef[1, l]
            - west_of(v, lane, lanes) * coef[2, l]
            + pltpu.roll(v, ring - 1, 1) * coef[5, l]
            - pltpu.roll(v, 1, 1) * coef[6, l]
            - up * ref[l + 2]
            - down * ref[l]
        )
        return v, off

    def off_adjoint(ref, l, up, down):
        v = ref[l + 1]
        off = (
            west_of(v, lane, lanes) * coef[3, l]
            - east_of(v, lane, lanes) * coef[0, l]
            + pltpu.roll(v, 1, 1) * coef[7, l]
            - pltpu.roll(v, ring - 1, 1) * coef[4, l]
            - up * ref[l + 2]
            - down * ref[l]
        )
        return v, off

    def resid_forward(x_ref, l):
        up, down, damp = level_terms(l)
        x, off = off_forward(x_ref, l, up, down)
        t = jnp.tanh(x)
        local = damp * (1.0 - t * t)
        diag = coef[8, l]
        r = x * diag + off + damp * t - cf[l]
        w = RELAXATION / (coef[9, l] + local)
        fw[l] = w
        fg[l] = 1.0 - w * (diag + local)
        fd[l] = -w * r
        fa[l + 1] = -w * r

    def resid_adjoint(m_ref, l):
        up, down, damp = level_terms(l)
        m, off = off_adjoint(m_ref, l, up, down)
        w = aw[l]
        d = carry_forcing[l] - (1.0 - ag[l]) * m - w * off
        ad2[l] = d
        aa[l + 1] = d

    def lin_forward(src, l):
        up, down, _ = level_terms(l)
        v, off = off_forward(src, l, up, down)
        return fg[l] * v + fd[l] - fw[l] * off

    def lin_adjoint(src, l, base):
        up, down, _ = level_terms(l)
        v, off = off_adjoint(src, l, up, down)
        return ag[l] * v + base[l] - aw[l] * off

    carry_forcing = ad
    ad2 = coef.at[9]

    def newton(x_ref, base):
        def sweep(f_src, f_dst, a_src, a_dst):
            def body(l, carry):
                f_dst[l + 1] = lin_forward(f_src, l)
                a_dst[l + 1] = lin_adjoint(a_src, l, base)
                return carry

            lax.fori_loop(0, levels, body, 0, unroll=8)

        pairs = [(fa, fb, aa, ab), (fb, fa, ab, aa)]
        for k in range(INNER - 2):
            sweep(*pairs[k % 2])
        return pairs[(INNER - 2) % 2]

    def first(l, carry):
        resid_forward(x0, l)
        return carry

    lax.fori_loop(0, levels, first, 0, unroll=8)
    last = newton(x0, ad)

    def close1(l, carry):
        xe, xw, me, mw = carry
        x = x0[l + 1, 0, :rows, :] + lin_forward(last[0], l)[0, :rows, :]
        m = lin_adjoint(last[2], l, ad)[0, :rows, :]
        x1[l + 1, 0, :rows, :] = x
        mu1[l + 1, 0, :rows, :] = m
        return pack(x, l, xe, xw) + pack(m, l, me, mw)

    xe, xw, me, mw = lax.fori_loop(0, levels, close1, (zero_tile,) * 4, unroll=8)
    pack1_e[0] = xe
    pack1_e[1] = me
    pack1_w[0] = xw
    pack1_w[1] = mw
    inside = pl.ds(1, levels)
    lon1 = lon_copies(
        pack1_e, pack1_w, recv1_e, recv1_w, sendl.at[pl.ds(6, 6)], gotl.at[pl.ds(6, 6)]
    )
    for copy in lon1[0]:
        copy.start()
    start(*lon1[1:])
    lat1 = lat_copies([x1.at[inside, 0], mu1.at[inside, 0]], send1, got1)
    start(*lat1)
    for copy in lon1[0]:
        copy.wait_recv()
    arrive(*lon1[1:])
    arrive(*lat1)

    def spread1(l, carry):
        x1[l + 1, 1] = unpack(recv1_e[0], recv1_w[0], l)
        mu1[l + 1, 1] = unpack(recv1_e[1], recv1_w[1], l)
        return carry

    lax.fori_loop(0, levels, spread1, 0, unroll=8)

    def second(l, carry):
        resid_forward(x1, l)
        resid_adjoint(mu1, l)
        return carry

    lax.fori_loop(0, levels, second, 0, unroll=8)
    last = newton(x1, ad2)

    for copy in late_loads:
        copy.wait()

    def close2(l, carry):
        xs = x1[l + 1, :, :rows, :] + lin_forward(last[0], l)[:, :rows, :]
        m = mu1[l + 1, 0, :rows, :] + lin_adjoint(last[2], l, ad2)[0, :rows, :]
        x2[l + 1, 0, :rows, :] = xs[0]
        x2[l + 1, 1, :rows, :] = xs[1]
        x = xs[0]
        state_out[l] = x
        adj_out[l] = m + weight_ref[l] * (x - obs_ref[l])
        return carry

    lax.fori_loop(0, levels, close2, 0, unroll=8)
    lat2 = (
        [
            remote(
                x2.at[inside, 0, pl.ds(rows - 1, 1), :],
                x2.at[inside, 0, pl.ds(ring - 1, 1), :],
                send2.at[0], got2.at[0], gx, north,
            )
        ],
        [
            remote(
                x2.at[inside, 0, pl.ds(0, 1), :],
                x2.at[inside, 0, pl.ds(rows, 1), :],
                send2.at[1], got2.at[1], gx, south,
            )
        ],
    )
    start(*lat2)
    stores = [
        pltpu.make_async_copy(state_out, state_h, load_sem.at[0]),
        pltpu.make_async_copy(adj_out, adj_h, load_sem.at[1]),
        pltpu.make_async_copy(resid_out, resid_h, load_sem.at[2]),
    ]
    stores[0].start()
    stores[1].start()
    arrive(*lat2)

    def finish(l, carry):
        up, down, damp = level_terms(l)
        x, off = off_forward(x2, l, up, down)
        r = x * coef[8, l] + off + damp * jnp.tanh(x) - cf[l]
        resid_out[l] = r[0, :rows, :]
        return carry

    lax.fori_loop(0, levels, finish, 0, unroll=8)
    stores[2].start()

    for up, down in lat0:
        flush(up, down)
    flush(*lat1)
    flush(*lat2)
    for copy in lon0[0] + lon1[0]:
        copy.wait_send()
    flush(*lon0[1:])
    flush(*lon1[1:])
    for copy in stores:
        copy.wait()


def hand_over(a, b, c, x, y, z, held, sem):
    takes = [pltpu.make_async_copy(ref, held.at[k], sem.at[k]) for k, ref in enumerate((a, b, c))]
    gives = [
        pltpu.make_async_copy(held.at[k], ref, sem.at[k + 3]) for k, ref in enumerate((x, y, z))
    ]
    for copy in takes:
        copy.start()
    for take, give in zip(takes, gives):
        take.wait()
        give.start()
    for copy in gives:
        copy.wait()


def solution(mesh):
    nx, ny = mesh.shape["gx"], mesh.shape["gy"]

    def per_device(*arrays):
        levels, rows, lanes = arrays[0].shape
        assert rows >= INNER and levels * (INNER + 1) <= lanes
        ring = 2 * rows
        out = jax.ShapeDtypeStruct((levels, rows, lanes), jnp.float32)
        hbm = pl.BlockSpec(memory_space=pltpu.HBM)
        f32 = jnp.float32

        def buf(*shape):
            return pltpu.VMEM(shape, f32)

        def padded():
            return buf(levels + 2, 2, ring, lanes)

        def full():
            return buf(levels, 2, ring, lanes)

        def dma(n):
            return pltpu.SemaphoreType.DMA((n,))

        results = pl.pallas_call(
            functools.partial(kernel, nx, ny),
            name="step_pair",
            out_shape=(out, out, out),
            in_specs=[hbm] * 13,
            out_specs=(hbm, hbm, hbm),
            scratch_shapes=[
                buf(levels, rows, lanes),
                buf(levels, rows, lanes),
                buf(levels, rows, lanes),
                buf(FIELDS, levels, ring, lanes),
                buf(FIELDS, rows, lanes),
                buf(FIELDS, rows, lanes),
                buf(FIELDS, ring, lanes),
                buf(FIELDS, ring, lanes),
                buf(2, rows, lanes),
                buf(2, rows, lanes),
                buf(2, ring, lanes),
                buf(2, ring, lanes),
                buf(10, levels, 2, ring, lanes),
                full(),
                padded(),
                padded(),
                padded(),
                padded(),
                full(),
                full(),
                full(),
                padded(),
                padded(),
                full(),
                full(),
                full(),
                padded(),
                padded(),
                buf(levels, rows, lanes),
                buf(levels, rows, lanes),
                pltpu.SMEM((levels,), f32),
                pltpu.SMEM((levels,), f32),
                pltpu.SMEM((1,), jnp.int32),
                dma(FIELDS + 5),
                dma(2 * FIELDS),
                dma(2 * FIELDS),
                dma(12),
                dma(12),
                dma(4),
                dma(4),
                dma(2),
                dma(2),
            ],
            compiler_params=pltpu.CompilerParams(
                collective_id=0, has_side_effects=True, vmem_limit_bytes=67043328
            ),
        )(*arrays)
        return pl.pallas_call(
            hand_over,
            name="hand_over",
            out_shape=(out, out, out),
            in_specs=[hbm] * 3,
            out_specs=(hbm, hbm, hbm),
            scratch_shapes=[buf(3, levels, rows, lanes), dma(6)],
            compiler_params=pltpu.CompilerParams(vmem_limit_bytes=67043328),
        )(*results)

    block = P(None, "gy", "gx")
    return jax.shard_map(
        per_device,
        mesh=mesh,
        in_specs=(block,) * 7 + (P(), P(), block, block, block, P()),
        out_specs=(block,) * 3,
        check_vma=False,
    )
```
